32 devices in a mesh: ctx: 8 (over z, core), head: 4 (over y, x).
Axes of the slice: x: 2, y: 2, z: 4, core: 2. Of those that a mesh axis runs over, the one named last changes fastest.
Arguments:
- q_latent: bfloat16 [1024, 128, 512], P('ctx', 'head'), may hold values from -4 to 4
- q_rope: bfloat16 [1024, 8192], P('ctx', 'head'), may hold values from -5 to 5
- latent: bfloat16 [1024, 512], P('ctx'), may hold values from -5 to 5
- key_rope: bfloat16 [1024, 64], P('ctx'), may hold values from -5 to 5
- out_grad: bfloat16 [1024, 128, 512], P('ctx', 'head'), may hold values from -5 to 5
- inputs: bfloat16 [1024, 7168], P('ctx', 'head'), may hold values from -5 to 5
- doc_ids: int32 [1024], replicated, may hold values from 0 to 7, never falling along the last dimension, each value on 1 to 256 neighbouring positions
Outputs:
- q_latent_grad: bfloat16 [1024, 128, 512], P('ctx', 'head')
- q_rope_grad: bfloat16 [1024, 8192], P('ctx', 'head')
- latent_grad: bfloat16 [1024, 512], P('ctx')
- key_rope_grad: bfloat16 [1024, 64], P('ctx')
- proj_grad: float32 [512, 7168], P('ctx', 'head')
The draws below stay inside these ranges and needn't reach their ends.
Inputs may be any that keep to these rules, and one draw needn't show every extreme that they name: `doc_ids`: ids never fall along the sequence; each document has at most 256 positions.
All inputs are finite; a program needn't handle non-finite values.
Results may differ from the reference program's by a relative error of at most 0.0058.
Values may be sent and summed in bfloat16 or wider, within the bound.
No kernel may reach another device: no remote copies, remote signals or barrier semaphores. Data moves between devices by JAX's collectives and lax.ppermute only.
A program may use at most 128 MiB of HBM per device.

```python
import math
import jax
import jax.numpy as jnp
import numpy as np
from jax import lax

D = 7168
HEADS = 128
KVL = 512
ROPE = 64
TOK_DEV = 128
WINDOW = 384
KEYS = 512
TOKENS = 1024
N_CTX = 8


def draw_latent(key, part):
    values = jnp.clip(jax.random.normal(jax.random.fold_in(key, 11), (TOKENS, KVL), jnp.float32), -5.0, 5.0)
    return values.astype(jnp.bfloat16)


def draw_q_latent(key, part):
    values = jnp.clip(0.5 * jax.random.normal(jax.random.fold_in(key, 13), (TOKENS, HEADS, KVL), jnp.float32), -4.0, 4.0)
    return values.astype(jnp.bfloat16)


def shard_levels(key, shape, shards, smallest, largest):
    factor_of, own = 1.0, jax.random.fold_in(key, 6)
    for position, shards_of in shards:
        heights = jnp.exp(jax.random.uniform(jax.random.fold_in(own, position), (shards_of,), jnp.float32, smallest / len(shards), largest / len(shards)))
        factor_of = factor_of * jnp.repeat(heights, shape[position] // shards_of).reshape([-1 if axis == position else 1 for axis in range(len(shape))])
    return factor_of


def profile(count, total, most, lean):
    loads = [(1 << 20) // math.isqrt(rank ** lean) + 1 for rank in range(2, count + 1)]
    rest, counts = total - most - (count - 1), [1] * (count - 1)
    while rest > 0:
        candidates = [i for i in range(count - 1) if counts[i] < most]
        mass, remaining = sum([loads[i] for i in candidates]), rest
        for i in candidates:
            addition = min(most - counts[i], max(1, remaining * loads[i] // mass), rest)
            counts[i] = counts[i] + addition
            rest = rest - addition
    return np.array([most] + counts)


def ragged_sizes(stream_key, number_of, total, most, slope):
    if number_of == 2:
        one = jax.random.randint(stream_key, (), max(1, total - most), min(most, total - 1) + 1)
        return jnp.stack([one, total - one])
    tallies = jnp.asarray(profile(number_of, total, most, slope), jnp.int32)
    twos = (number_of - 1) // 2
    giver, taker = tallies[1:1 + 2 * twos:2], tallies[2:2 + 2 * twos:2]
    slack = jnp.minimum(giver - 1, most - taker)
    passed = jax.random.randint(jax.random.fold_in(stream_key, 1), (twos,), 0, 1 << 20) % (slack + 1)
    tallies = tallies.at[1:1 + 2 * twos:2].set(giver - passed).at[2:2 + 2 * twos:2].set(taker + passed)
    return tallies[jax.random.permutation(jax.random.fold_in(stream_key, 2), number_of)]


def gaussian(own_key, extent, scale, bound, split=(), kind=jnp.bfloat16):
    array = scale * jax.random.normal(own_key, extent, jnp.float32)
    if split:
        array = array * shard_levels(own_key, extent, split, -0.22, 0.18)
    return jnp.clip(array, -bound, bound).astype(kind)


def setup_inputs(seed: int = 0) -> dict:
    keys = jax.random.split(jax.random.key(seed), 8)
    return {
        "q_latent": draw_q_latent(jax.random.fold_in(keys[7], 71), 0),
        "q_rope": gaussian(keys[1], (TOKENS, HEADS * ROPE), 1.0, 5.0, ((0, 8), (1, 4))),
        "latent": draw_latent(jax.random.fold_in(keys[7], 71), 0),
        "key_rope": gaussian(keys[3], (TOKENS, ROPE), 1.0, 5.0, ((0, 8),)),
        "out_grad": gaussian(keys[4], (TOKENS, HEADS, KVL), 1.0, 5.0, ((0, 8), (1, 4))),
        "inputs": gaussian(keys[5], (TOKENS, D), 1.0, 5.0, ((0, 8), (1, 4))),
        "doc_ids": jnp.searchsorted(jnp.cumsum(ragged_sizes(keys[6], 8, TOKENS, TOKENS // 4, 1)), jnp.arange(TOKENS), side="right").astype(jnp.int32),
    }


softmax_scale = 192.0 ** -0.5


def reference(q_latent, q_rope, latent, key_rope, out_grad, inputs, doc_ids):
    lat_pad = jnp.concatenate([jnp.zeros((WINDOW, KVL), jnp.float32), latent.astype(jnp.float32)], axis=0)
    rope_pad = jnp.concatenate([jnp.zeros((WINDOW, ROPE), jnp.float32), key_rope.astype(jnp.float32)], axis=0)
    doc_pad = jnp.concatenate([jnp.full((WINDOW,), -1, jnp.int32), doc_ids.astype(jnp.int32)], axis=0)
    qrope_all = q_rope.reshape(TOKENS, HEADS, ROPE)

    def block_step(carry, block):
        acc_lat, acc_rope = carry
        start = (block * TOK_DEV).astype(jnp.int32)
        qlat = lax.dynamic_slice_in_dim(q_latent, start, TOK_DEV, 0).astype(jnp.float32)
        qrot = lax.dynamic_slice_in_dim(qrope_all, start, TOK_DEV, 0).astype(jnp.float32)
        grad_out = lax.dynamic_slice_in_dim(out_grad, start, TOK_DEV, 0).astype(jnp.float32)
        keys_lat = lax.dynamic_slice_in_dim(lat_pad, start, KEYS, 0)
        keys_rope = lax.dynamic_slice_in_dim(rope_pad, start, KEYS, 0)
        key_doc = lax.dynamic_slice_in_dim(doc_pad, start, KEYS, 0)
        query_doc = lax.dynamic_slice_in_dim(doc_ids.astype(jnp.int32), start, TOK_DEV, 0)
        qpos = jnp.arange(TOK_DEV, dtype=jnp.int32)
        kpos = jnp.arange(KEYS, dtype=jnp.int32) - WINDOW
        allowed = (kpos[None, :] <= qpos[:, None]) & (qpos[:, None] - kpos[None, :] < WINDOW) & (key_doc[None, :] == query_doc[:, None])
        scores = (jnp.einsum("thj,kj->thk", qlat, keys_lat) + jnp.einsum("thr,kr->thk", qrot, keys_rope)) * softmax_scale
        masked = jnp.where(allowed[:, None, :], scores, -jnp.inf)
        top = jnp.max(masked, axis=-1, keepdims=True)
        expo = jnp.exp(masked - top)
        probs = expo / jnp.sum(expo, axis=-1, keepdims=True)
        probs_low = lax.optimization_barrier(probs.astype(jnp.bfloat16)).astype(jnp.float32)
        merged = jnp.einsum("thk,kj->thj", probs_low, keys_lat)
        delta = jnp.sum(grad_out * merged, axis=-1)
        dprob = jnp.einsum("thj,kj->thk", grad_out, keys_lat)
        dscore = (probs * (dprob - delta[..., None]) * softmax_scale)
        dscore = lax.optimization_barrier(dscore.astype(jnp.bfloat16)).astype(jnp.float32)
        grad_qlat = jnp.einsum("thk,kj->thj", dscore, keys_lat).astype(jnp.bfloat16)
        grad_qrope = jnp.einsum("thk,kr->thr", dscore, keys_rope).reshape(TOK_DEV, HEADS * ROPE).astype(jnp.bfloat16)
        part_lat = jnp.einsum("thk,thj->kj", dscore, qlat) + jnp.einsum("thk,thj->kj", probs_low, grad_out)
        part_rope = jnp.einsum("thk,thr->kr", dscore, qrot)
        acc_lat = lax.dynamic_update_slice_in_dim(acc_lat, lax.dynamic_slice_in_dim(acc_lat, start, KEYS, 0) + part_lat, start, 0)
        acc_rope = lax.dynamic_update_slice_in_dim(acc_rope, lax.dynamic_slice_in_dim(acc_rope, start, KEYS, 0) + part_rope, start, 0)
        return (acc_lat, acc_rope), (grad_qlat, grad_qrope)

    init = (jnp.zeros((WINDOW + TOKENS, KVL), jnp.float32), jnp.zeros((WINDOW + TOKENS, ROPE), jnp.float32))
    (acc_lat, acc_rope), (grads_qlat, grads_qrope) = lax.scan(block_step, init, jnp.arange(N_CTX, dtype=jnp.int32))
    q_latent_grad = grads_qlat.reshape(TOKENS, HEADS, KVL)
    q_rope_grad = grads_qrope.reshape(TOKENS, HEADS * ROPE)
    latent_grad = acc_lat[WINDOW:].astype(jnp.bfloat16)
    key_rope_grad = acc_rope[WINDOW:].astype(jnp.bfloat16)
    proj_grad = jnp.dot(latent_grad.T, inputs, preferred_element_type=jnp.float32)
    return q_latent_grad, q_rope_grad, latent_grad, key_rope_grad, proj_grad
```

```python
import functools

import jax
import jax.numpy as jnp
from jax import lax
from jax.experimental import pallas as pl
from jax.experimental.pallas import tpu as pltpu
from jax.sharding import PartitionSpec as P


WIN_BLK = 3
DOCS = 4
CHUNK = 16
PAIR = 2
LANES = 128
DOC_VALUES = 8

softmax_scale = 192.0 ** (-0.5)


def nt(a, b):
    return lax.dot_general(a, b, (((1,), (1,)), ((), ())), preferred_element_type=jnp.float32)


def nn(a, b):
    return lax.dot_general(a, b, (((1,), (0,)), ((), ())), preferred_element_type=jnp.float32)


def tn(a, b):
    return lax.dot_general(a, b, (((0,), (0,)), ((), ())), preferred_element_type=jnp.float32)


def pack_kernel(lat_ref, rope_ref, out_ref):
    lat = lat_ref.shape[1]
    out_ref[:, :lat] = lat_ref[...]
    out_ref[:, lat:] = rope_ref[...].astype(jnp.float32).T.astype(out_ref.dtype)


def score_step(begin, keys_ref, first_ref, q_ref, qr_ref, do_ref, ds_ref, acc_ref, turn_ref, *, width, lat, heads, window):
    keys = keys_ref[pl.ds(begin, width), :]
    klat = keys[:, :lat]
    q = q_ref[...]
    do = do_ref[...]
    block = q.shape[0]
    rope = turn_ref.shape[1]
    turned = qr_ref[...].astype(jnp.float32)
    for head in range(heads):
        turn_ref[pl.ds(head, CHUNK, stride=heads), :] = turned[:, head * rope:(head + 1) * rope]
    qr = turn_ref[...].astype(jnp.bfloat16)
    firsts = []
    lasts = []
    for at in range(0, block, LANES):
        token = begin + (lax.broadcasted_iota(jnp.int32, first_ref.shape, 1) + at) // heads
        firsts.append(jnp.take_along_axis(first_ref[...], token, axis=1, mode="promise_in_bounds")[:1])
        lasts.append(token[:1] + window)
    first = jnp.concatenate(firsts, axis=1)
    last = jnp.concatenate(lasts, axis=1)
    scores = nt(klat, q) + nt(keys[:, lat:], qr)
    pos = lax.broadcasted_iota(jnp.int32, scores.shape, 0) + begin
    allowed = (pos >= first) & (pos <= last)
    scores = jnp.where(allowed, scores, -jnp.inf)
    top = jnp.max(scores, axis=0, keepdims=True)
    expo = jnp.exp((scores - top) * softmax_scale)
    inverse = 1.0 / jnp.sum(expo, axis=0, keepdims=True)
    probs = expo * inverse
    low = probs.astype(jnp.bfloat16)
    dprob = nt(klat, do)
    delta = jnp.sum(low.astype(jnp.float32) * dprob, axis=0, keepdims=True)
    ds = (probs * (dprob - delta) * softmax_scale).astype(jnp.bfloat16)
    ds_ref[0] = ds
    acc_ref[pl.ds(begin, width), :lat] += nn(ds, q) + nn(low, do)
    acc_ref[pl.ds(begin, width), lat:] += nn(ds, qr)


def score_kernel(place_ref, doc_ref, q_ref, qr_ref, do_ref, *refs, width, lat, heads, window):
    blocks, (ds_ref, keys_ref, acc_ref, first_ref, turn_ref) = refs[:-5], refs[-5:]
    tok = blocks[0].shape[0]
    step = pl.program_id(0)

    @pl.when(step == 0)
    def _():
        acc_ref[...] = jnp.zeros_like(acc_ref)
        for slot, packed in enumerate(blocks):
            keys_ref[slot * tok:(slot + 1) * tok, :] = packed[...]
        rank = place_ref[0]
        ids = doc_ref[...]
        mine = doc_ref[pl.ds(rank, 1), :]
        begins = jnp.zeros(mine.shape, jnp.float32)
        for value in range(DOC_VALUES - 1):
            count = jnp.sum(jnp.where(ids == value, 1.0, 0.0), axis=0, keepdims=True)
            count = jnp.sum(count, axis=1, keepdims=True)
            begins += jnp.where(mine > value, count, 0.0)
        here = lax.broadcasted_iota(jnp.int32, mine.shape, 1) + rank * tok
        first = jnp.maximum(begins.astype(jnp.int32), here - (window - 1)) - (rank * tok - window)
        first_ref[...] = jnp.broadcast_to(first, first_ref.shape)

    begin = pl.multiple_of(step * CHUNK, CHUNK)
    score_step(begin, keys_ref, first_ref, q_ref, qr_ref, do_ref, ds_ref, acc_ref, turn_ref,
               width=width, lat=lat, heads=heads, window=window)


def score_more_kernel(first_ref, q_ref, qr_ref, do_ref, keys_ref, had_ref, *refs, width, lat, heads, window, offset):
    ds_ref, part_refs, acc_ref, turn_ref = refs[0], refs[1:-2], refs[-2], refs[-1]
    step = pl.program_id(0)

    @pl.when(step == 0)
    def _():
        acc_ref[...] = had_ref[...]

    begin = pl.multiple_of((step + offset) * CHUNK, CHUNK)
    score_step(begin, keys_ref, first_ref, q_ref, qr_ref, do_ref, ds_ref, acc_ref, turn_ref,
               width=width, lat=lat, heads=heads, window=window)

    @pl.when(step == pl.num_programs(0) - 1)
    def _():
        for slot, part_ref in enumerate(part_refs):
            tok = part_ref.shape[0]
            part_ref[...] = acc_ref[slot * tok:(slot + 1) * tok, :].astype(part_ref.dtype)


def query_kernel(ds_ref, keys_ref, *refs, width, lat, heads, offset):
    dq_ref, dqr_ref, turn_ref = refs[-3:]
    begin = pl.multiple_of((pl.program_id(0) + offset) * CHUNK, CHUNK)
    keys = keys_ref[pl.ds(begin, width), :]
    ds = ds_ref[0]
    dq_ref[...] = tn(ds, keys[:, :lat]).astype(dq_ref.dtype)
    turn_ref[...] = tn(ds, keys[:, lat:])
    rope = turn_ref.shape[1]
    for head in range(0, heads, 2):
        pair = [turn_ref[pl.ds(head + which, CHUNK, stride=heads), :] for which in range(2)]
        dqr_ref[:, head * rope:(head + 2) * rope] = jnp.concatenate(pair, axis=1).astype(dqr_ref.dtype)


def proj_kernel(place_ref, index_ref, *refs, groups):
    pieces, fed, out_ref, all_ref = refs[:groups], refs[groups:-2], refs[-2], refs[-1]
    half = out_ref.shape[1]
    all_ref[groups] = jnp.zeros(all_ref.shape[1:], all_ref.dtype)
    for by, piece in enumerate(pieces):
        all_ref[(place_ref[1] - by + groups) % groups] = piece[...]
    lefts = [all_ref[index_ref[k]] for k in range(len(fed))]
    span = out_ref.shape[2]
    for at in range(0, span, 2 * LANES):
        lanes = slice(at, min(at + 2 * LANES, span))
        product = tn(lefts[0], fed[0][:, lanes])
        for left, right in zip(lefts[1:], fed[1:]):
            product += tn(left, right[:, lanes])
        for core in range(PAIR):
            out_ref[place_ref[0] ^ core, :, lanes] = product[core * half:(core + 1) * half]


def ring(peers, by):
    return [(i, (i + by) % peers) for i in range(peers)]


def line(groups, stage, edge):
    pairs = []
    for left in range(edge, groups - 1, 2):
        if left + 1 - stage >= 0:
            pairs.append((left, left + 1))
        if left + stage < groups:
            pairs.append((left + 1, left))
    return pairs


def across(peers, by):
    return [(i, i ^ by) for i in range(peers)]


def stride_ring(peers, by):
    return [(i, (i + PAIR * by) % peers) for i in range(peers)]


def in_hbm(array):
    return pltpu.with_memory_space_constraint(array, pltpu.HBM)


def shards(q_latent, q_rope, latent, key_rope, out_grad, inputs, doc_ids):
    tok, heads, lat = q_latent.shape
    rope = key_rope.shape[1]
    total = doc_ids.shape[0]
    ctxs = lax.axis_size("ctx")
    headers = lax.axis_size("head")
    window = min(WIN_BLK * tok, total // DOCS)
    depth = window // tok
    slots = depth + 1
    rank = lax.axis_index("ctx")
    rows = tok * heads
    steps = tok // CHUNK
    block = CHUNK * heads
    keyed = lat + rope
    groups = ctxs // PAIR
    low = jnp.bfloat16
    smem = pl.BlockSpec(memory_space=pltpu.SMEM)
    whole_of = pl.BlockSpec(memory_space=pltpu.VMEM)

    packed = pl.pallas_call(
        pack_kernel,
        in_specs=[whole_of, whole_of],
        out_specs=whole_of,
        out_shape=jax.ShapeDtypeStruct((tok, keyed), low),
        name="pack",
    )(latent, key_rope.T)
    earlier = [lax.ppermute(packed, "ctx", ring(ctxs, back)) for back in range(depth, 0, -1)]
    fed, source = [inputs], [rank // PAIR]
    flows = [inputs, inputs]
    for stage in range(1, groups):
        moved = []
        for edge in range(2):
            pairs = line(groups, stage, edge)
            if not pairs:
                moved.append(None)
                continue
            moved.append(lax.ppermute(flows[1 - edge], "ctx", [(PAIR * a + c, PAIR * b + c) for a, b in pairs for c in range(PAIR)]))
            fed.append(moved[edge])
            ahead = (rank // PAIR) % 2 == edge
            origin = rank // PAIR + jnp.where(ahead, stage, -stage)
            source.append(jnp.where((origin >= 0) & (origin < groups), origin, groups))
        flows = moved

    q = q_latent.reshape(rows, lat)
    do = out_grad.reshape(rows, lat)
    span = window + tok
    width = window + CHUNK
    places = rank.astype(jnp.int32).reshape(1)
    split = steps // 2
    resident = lambda *shape: pl.BlockSpec(shape, lambda i: (0,) * len(shape))
    limits = pltpu.CompilerParams(dimension_semantics=("arbitrary",), vmem_limit_bytes=32 * 1024 * 1024)
    sizes = dict(width=width, lat=lat, heads=heads, window=window)
    cost = pl.CostEstimate(flops=rows * width * (5 * lat), transcendentals=0, bytes_accessed=6 << 20)

    def tiles(offset):
        return [
            pl.BlockSpec((block, lat), lambda i: (i + offset, 0)),
            pl.BlockSpec((CHUNK, heads * rope), lambda i: (i + offset, 0)),
            pl.BlockSpec((block, lat), lambda i: (i + offset, 0)),
        ]

    chunk_of = pl.BlockSpec((1, width, block), lambda i: (i, 0, 0))
    ds_shape = jax.ShapeDtypeStruct((split, width, block), low)
    turner = pltpu.VMEM((block, rope), jnp.float32)
    streams = (in_hbm(q), in_hbm(q_rope), in_hbm(do))
    ds0, keys, acc, first = pl.pallas_call(
        functools.partial(score_kernel, **sizes),
        grid=(split,),
        in_specs=[smem, resident(ctxs, tok)] + tiles(0) + [resident(tok, keyed)] * slots,
        out_specs=[chunk_of, resident(span, keyed), resident(span, keyed), resident(8, tok)],
        out_shape=[
            ds_shape,
            jax.ShapeDtypeStruct((span, keyed), low),
            jax.ShapeDtypeStruct((span, keyed), jnp.float32),
            jax.ShapeDtypeStruct((8, tok), jnp.int32),
        ],
        scratch_shapes=[turner],
        compiler_params=limits,
        cost_estimate=cost,
        name="score0",
    )(places, doc_ids.reshape(ctxs, tok), *streams, *earlier, packed)
    ds1, *part = pl.pallas_call(
        functools.partial(score_more_kernel, offset=split, **sizes),
        grid=(split,),
        in_specs=[resident(8, tok)] + tiles(split) + [resident(span, keyed)] * 2,
        out_specs=[chunk_of] + [resident(tok, keyed)] * slots,
        out_shape=[ds_shape] + [jax.ShapeDtypeStruct((tok, keyed), low)] * depth
        + [jax.ShapeDtypeStruct((tok, keyed), jnp.float32)],
        scratch_shapes=[pltpu.VMEM((span, keyed), jnp.float32), turner],
        compiler_params=limits,
        cost_estimate=cost,
        name="score1",
    )(first, *streams, keys, acc)

    shapes = [jax.ShapeDtypeStruct((rows, lat), low), jax.ShapeDtypeStruct((tok, heads * rope), low)]
    grads = ()
    for call, ds in enumerate((ds0, ds1)):
        offset = call * split
        grads = pl.pallas_call(
            functools.partial(query_kernel, width=width, lat=lat, heads=heads, offset=offset),
            grid=(split,),
            in_specs=[chunk_of, resident(span, keyed)] + [pl.BlockSpec(memory_space=pl.ANY)] * len(grads),
            out_specs=tiles(offset)[:2],
            out_shape=shapes,
            scratch_shapes=[turner],
            input_output_aliases={2: 0, 3: 1} if call else {},
            compiler_params=limits,
            cost_estimate=pl.CostEstimate(flops=rows * width * lat, transcendentals=0, bytes_accessed=4 << 20),
            name="query",
        )(ds, keys, *[in_hbm(grad) for grad in grads])
    q_latent_grad = grads[0].reshape(tok, heads, lat)
    q_rope_grad = grads[1]

    mine = part[depth]
    for back in range(1, depth + 1):
        mine = mine + lax.ppermute(part[depth - back], "ctx", ring(ctxs, -back)).astype(jnp.float32)
    sent = mine.astype(low)
    whole = mine
    for by in range(1, headers):
        whole = whole + lax.ppermute(sent, "head", across(headers, by)).astype(jnp.float32)
    found = whole.astype(low)
    latent_grad = found[:, :lat]
    key_rope_grad = found[:, lat:]

    narrow = PAIR * lat // ctxs
    mine_at = rank // PAIR
    pieces = []
    for by in range(groups):
        piece = lax.dynamic_slice_in_dim(found, ((mine_at + by) % groups) * narrow, narrow, 1)
        pieces.append(lax.ppermute(piece, "ctx", stride_ring(ctxs, by)) if by else piece)
    words = jnp.stack([rank % PAIR, mine_at]).astype(jnp.int32)
    width_in = inputs.shape[1]
    product = pl.pallas_call(
        functools.partial(proj_kernel, groups=groups),
        in_specs=[smem, smem] + [whole_of] * (groups + len(fed)),
        out_specs=whole_of,
        out_shape=jax.ShapeDtypeStruct((PAIR, lat // ctxs, width_in), jnp.float32),
        scratch_shapes=[pltpu.VMEM((groups + 1, tok, narrow), low)],
        compiler_params=pltpu.CompilerParams(vmem_limit_bytes=24 * 1024 * 1024),
        name="proj",
    )(words, jnp.stack(source).astype(jnp.int32), *pieces, *fed)
    proj_grad = product[0] + lax.ppermute(product[1], "ctx", across(ctxs, 1))
    return (q_latent_grad, q_rope_grad, latent_grad, key_rope_grad, proj_grad)


def solution(mesh):
    placed = (
        P("ctx", "head", None),
        P("ctx", "head"),
        P("ctx", None),
        P("ctx", None),
        P("ctx", "head", None),
        P("ctx", "head"),
        P(),
    )

    return jax.shard_map(
        shards,
        mesh=mesh,
        in_specs=placed,
        out_specs=(
            P("ctx", "head", None),
            P("ctx", "head"),
            P("ctx", None),
            P("ctx", None),
            P("ctx", "head"),
        ),
        check_vma=False,
    )
```

```python
import functools

import jax
import jax.numpy as jnp
from jax import lax
from jax.experimental import pallas as pl
from jax.experimental.pallas import tpu as pltpu
from jax.sharding import PartitionSpec as P


WIN_BLK = 3
DOCS = 4
CHUNK = 16
PAIR = 2
LANES = 128
DOC_VALUES = 8

softmax_scale = 192.0 ** (-0.5)


def nt(a, b):
    return lax.dot_general(a, b, (((1,), (1,)), ((), ())), preferred_element_type=jnp.float32)


def nn(a, b):
    return lax.dot_general(a, b, (((1,), (0,)), ((), ())), preferred_element_type=jnp.float32)


def tn(a, b):
    return lax.dot_general(a, b, (((0,), (0,)), ((), ())), preferred_element_type=jnp.float32)


def score_step(begin, keys_ref, first_ref, q_ref, qr_ref, do_ref, ds_ref, acc_ref, turn_ref, *, width, lat, heads, window):
    keys = keys_ref[pl.ds(begin, width), :]
    klat = keys[:, :lat]
    q = q_ref[...]
    do = do_ref[...]
    block = q.shape[0]
    rope = turn_ref.shape[1]
    turned = qr_ref[...].astype(jnp.float32)
    for head in range(heads):
        turn_ref[pl.ds(head, CHUNK, stride=heads), :] = turned[:, head * rope:(head + 1) * rope]
    qr = turn_ref[...].astype(jnp.bfloat16)
    firsts = []
    lasts = []
    for at in range(0, block, LANES):
        token = begin + (lax.broadcasted_iota(jnp.int32, first_ref.shape, 1) + at) // heads
        firsts.append(jnp.take_along_axis(first_ref[...], token, axis=1, mode="promise_in_bounds")[:1])
        lasts.append(token[:1] + window)
    first = jnp.concatenate(firsts, axis=1)
    last = jnp.concatenate(lasts, axis=1)
    scores = nt(klat, q) + nt(keys[:, lat:], qr)
    pos = lax.broadcasted_iota(jnp.int32, scores.shape, 0) + begin
    allowed = (pos >= first) & (pos <= last)
    scores = jnp.where(allowed, scores, -jnp.inf)
    top = jnp.max(scores, axis=0, keepdims=True)
    expo = jnp.exp((scores - top) * softmax_scale)
    inverse = 1.0 / jnp.sum(expo, axis=0, keepdims=True)
    probs = expo * inverse
    low = probs.astype(jnp.bfloat16)
    dprob = nt(klat, do)
    delta = jnp.sum(low.astype(jnp.float32) * dprob, axis=0, keepdims=True)
    ds = (probs * (dprob - delta) * softmax_scale).astype(jnp.bfloat16)
    ds_ref[0] = ds
    acc_ref[pl.ds(begin, width), :lat] += nn(ds, q) + nn(low, do)
    acc_ref[pl.ds(begin, width), lat:] += nn(ds, qr)


def score_kernel(place_ref, doc_ref, q_ref, qr_ref, do_ref, *refs, width, lat, heads, window, slots):
    blocks, ropes, refs = refs[:slots], refs[slots:2 * slots], refs[2 * slots:]
    (ds_ref, keys_ref), part_refs, (acc_ref, first_ref, turn_ref) = refs[:2], refs[2:-3], refs[-3:]
    tok = blocks[0].shape[0]
    step = pl.program_id(0)

    @pl.when(step == 0)
    def _():
        acc_ref[...] = jnp.zeros_like(acc_ref)
        for slot in range(slots):
            rows = slice(slot * tok, (slot + 1) * tok)
            keys_ref[rows, :lat] = blocks[slot][...]
            keys_ref[rows, lat:] = ropes[slot][...].astype(jnp.float32).T.astype(keys_ref.dtype)
        rank = place_ref[0]
        ids = doc_ref[...]
        mine = doc_ref[pl.ds(rank, 1), :]
        begins = jnp.zeros(mine.shape, jnp.float32)
        for value in range(DOC_VALUES - 1):
            count = jnp.sum(jnp.where(ids == value, 1.0, 0.0), axis=0, keepdims=True)
            count = jnp.sum(count, axis=1, keepdims=True)
            begins += jnp.where(mine > value, count, 0.0)
        here = lax.broadcasted_iota(jnp.int32, mine.shape, 1) + rank * tok
        first = jnp.maximum(begins.astype(jnp.int32), here - (window - 1)) - (rank * tok - window)
        first_ref[...] = jnp.broadcast_to(first, first_ref.shape)

    begin = pl.multiple_of(step * CHUNK, CHUNK)
    score_step(begin, keys_ref, first_ref, q_ref, qr_ref, do_ref, ds_ref, acc_ref, turn_ref,
               width=width, lat=lat, heads=heads, window=window)

    @pl.when(step == pl.num_programs(0) - 1)
    def _():
        for slot, part_ref in enumerate(part_refs):
            part_ref[...] = acc_ref[slot * tok:(slot + 1) * tok, :].astype(part_ref.dtype)


def query_kernel(ds_ref, keys_ref, *refs, width, lat, heads, offset):
    dq_ref, dqr_ref, turn_ref = refs[-3:]
    begin = pl.multiple_of((pl.program_id(0) + offset) * CHUNK, CHUNK)
    keys = keys_ref[pl.ds(begin, width), :]
    ds = ds_ref[0]
    dq_ref[...] = tn(ds, keys[:, :lat]).astype(dq_ref.dtype)
    turn_ref[...] = tn(ds, keys[:, lat:])
    rope = turn_ref.shape[1]
    for head in range(0, heads, 2):
        pair = [turn_ref[pl.ds(head + which, CHUNK, stride=heads), :] for which in range(2)]
        dqr_ref[:, head * rope:(head + 2) * rope] = jnp.concatenate(pair, axis=1).astype(dqr_ref.dtype)


def proj_kernel(place_ref, own_ref, mail_ref, here_ref, near_ref, keep_ref, give_ref):
    count, half, span = keep_ref.shape
    north = place_ref[0] == 1
    own = own_ref[...]
    mail = mail_ref[...]
    for at in range(0, span, 2 * LANES):
        lanes = slice(at, min(at + 2 * LANES, span))
        product = tn(own, here_ref[:, lanes]) + tn(mail, near_ref[:, lanes])
        for group in range(count):
            low = product[PAIR * group * half:(PAIR * group + 1) * half]
            high = product[(PAIR * group + 1) * half:(PAIR * group + 2) * half]
            keep_ref[place_ref[1] ^ group, :, lanes] = jnp.where(north, high, low)
            give_ref[place_ref[1] ^ group, :, lanes] = jnp.where(north, low, high).astype(give_ref.dtype)


def ring(peers, by):
    return [(i, (i + by) % peers) for i in range(peers)]


def across(peers, by):
    return [(i, i ^ by) for i in range(peers)]


def in_hbm(array):
    return pltpu.with_memory_space_constraint(array, pltpu.HBM)


def shards(q_latent, q_rope, latent, key_rope, out_grad, inputs, doc_ids):
    tok, heads, lat = q_latent.shape
    rope = key_rope.shape[1]
    total = doc_ids.shape[0]
    ctxs = lax.axis_size("ctx")
    headers = lax.axis_size("head")
    window = min(WIN_BLK * tok, total // DOCS)
    depth = window // tok
    slots = depth + 1
    rank = lax.axis_index("ctx")
    rows = tok * heads
    steps = tok // CHUNK
    block = CHUNK * heads
    keyed = lat + rope
    groups = ctxs // PAIR
    low = jnp.bfloat16
    smem = pl.BlockSpec(memory_space=pltpu.SMEM)
    whole_of = pl.BlockSpec(memory_space=pltpu.VMEM)

    blocks = [lax.ppermute(latent, "ctx", ring(ctxs, back)) for back in range(depth, 0, -1)] + [latent]
    turned = key_rope.T
    ropes = [lax.ppermute(turned, "ctx", ring(ctxs, back)) for back in range(depth, 0, -1)] + [turned]
    near = lax.ppermute(inputs, "ctx", across(ctxs, PAIR))

    q = q_latent.reshape(rows, lat)
    do = out_grad.reshape(rows, lat)
    span = window + tok
    width = window + CHUNK
    places = rank.astype(jnp.int32).reshape(1)
    split = steps // 2
    resident = lambda *shape: pl.BlockSpec(shape, lambda i: (0,) * len(shape))
    limits = pltpu.CompilerParams(dimension_semantics=("arbitrary",), vmem_limit_bytes=20 * 1024 * 1024)
    sizes = dict(width=width, lat=lat, heads=heads, window=window)

    def tiles(offset):
        return [
            pl.BlockSpec((block, lat), lambda i: (i + offset, 0)),
            pl.BlockSpec((CHUNK, heads * rope), lambda i: (i + offset, 0)),
            pl.BlockSpec((block, lat), lambda i: (i + offset, 0)),
        ]

    turner = pltpu.VMEM((block, rope), jnp.float32)
    ds, keys, *part = pl.pallas_call(
        functools.partial(score_kernel, slots=slots, **sizes),
        grid=(steps,),
        in_specs=[smem, resident(ctxs, tok)] + tiles(0) + [resident(tok, lat)] * slots + [resident(rope, tok)] * slots,
        out_specs=[pl.BlockSpec((1, width, block), lambda i: (i, 0, 0)), resident(span, keyed)] + [resident(tok, keyed)] * slots,
        out_shape=[jax.ShapeDtypeStruct((steps, width, block), low), jax.ShapeDtypeStruct((span, keyed), low)]
        + [jax.ShapeDtypeStruct((tok, keyed), low)] * slots,
        scratch_shapes=[pltpu.VMEM((span, keyed), jnp.float32), pltpu.VMEM((8, tok), jnp.int32), turner],
        compiler_params=limits,
        name="score",
    )(places, in_hbm(doc_ids.reshape(ctxs, tok)), in_hbm(q), in_hbm(q_rope), in_hbm(do), *blocks[:-1], in_hbm(latent), *ropes[:-1], in_hbm(turned))

    shapes = [jax.ShapeDtypeStruct((rows, lat), low), jax.ShapeDtypeStruct((tok, heads * rope), low)]
    grads = ()
    for call in range(2):
        offset = call * split
        grads = pl.pallas_call(
            functools.partial(query_kernel, width=width, lat=lat, heads=heads, offset=offset),
            grid=(split,),
            in_specs=[pl.BlockSpec((1, width, block), lambda i, offset=offset: (i + offset, 0, 0)), resident(span, keyed)] + [pl.BlockSpec(memory_space=pl.ANY)] * len(grads),
            out_specs=tiles(offset)[:2],
            out_shape=shapes,
            scratch_shapes=[turner],
            input_output_aliases={2: 0, 3: 1} if call else {},
            compiler_params=pltpu.CompilerParams(dimension_semantics=("arbitrary",), vmem_limit_bytes=10 * 1024 * 1024),
            name="query",
        )(ds, keys, *[in_hbm(grad) for grad in grads])
    q_latent_grad = grads[0].reshape(tok, heads, lat)
    q_rope_grad = grads[1]

    mine = part[depth].astype(jnp.float32)
    for back in range(1, depth + 1):
        mine = mine + lax.ppermute(part[depth - back], "ctx", ring(ctxs, -back)).astype(jnp.float32)
    sent = lax.optimization_barrier(mine.astype(low))
    terms = [sent.astype(jnp.float32)]
    for by in range(1, headers):
        terms.append(lax.ppermute(sent, "head", across(headers, by)).astype(jnp.float32))
    while len(terms) > 1:
        terms = [left + right for left, right in zip(terms[::2], terms[1::2])]
    found = terms[0].astype(low)
    latent_grad = found[:, :lat]
    key_rope_grad = found[:, lat:]

    narrow = PAIR * lat // ctxs
    count = groups // 2
    odd = (rank // PAIR) % 2

    def columns(parity):
        taken = [lax.dynamic_slice_in_dim(found, (2 * group + parity) * narrow, narrow, 1) for group in range(count)]
        return jnp.concatenate(taken, axis=1)

    mail = lax.ppermute(columns(1 - odd), "ctx", across(ctxs, PAIR))
    words = jnp.stack([rank % PAIR, rank // (2 * PAIR)]).astype(jnp.int32)
    half, width_in = lat // ctxs, inputs.shape[1]
    keep, give = pl.pallas_call(
        proj_kernel,
        in_specs=[smem] + [whole_of] * 4,
        out_specs=[whole_of] * 2,
        out_shape=[jax.ShapeDtypeStruct((count, half, width_in), jnp.float32), jax.ShapeDtypeStruct((count, half, width_in), low)],
        compiler_params=pltpu.CompilerParams(vmem_limit_bytes=24 * 1024 * 1024),
        name="proj",
    )(words, columns(odd), mail, inputs, near)
    keep = keep + lax.ppermute(give, "ctx", across(ctxs, 1)).astype(jnp.float32)
    while count > 1:
        count //= 2
        keep = keep[:count] + lax.ppermute(keep[count:].astype(low), "ctx", across(ctxs, 2 * PAIR * count)).astype(jnp.float32)
    proj_grad = keep[0]
    return (q_latent_grad, q_rope_grad, latent_grad, key_rope_grad, proj_grad)


def solution(mesh):
    placed = (
        P("ctx", "head", None),
        P("ctx", "head"),
        P("ctx", None),
        P("ctx", None),
        P("ctx", "head", None),
        P("ctx", "head"),
        P(),
    )

    return jax.shard_map(
        shards,
        mesh=mesh,
        in_specs=placed,
        out_specs=(
            P("ctx", "head", None),
            P("ctx", "head"),
            P("ctx", None),
            P("ctx", None),
            P("ctx", "head"),
        ),
        check_vma=False,
    )
```
